256 devices in a mesh: gx: 32 (over y, z_lo, core), gy: 8 (over x, z_hi).
Axes of the slice: x: 4, y: 4, z: 8 (z_hi: 2, z_lo: 4; z = z_hi * 4 + z_lo), core: 2. Of those that a mesh axis runs over, the one named last changes fastest.
Arguments:
- signal: float32 [45, 32, 64, 128], P(None, 'gx', 'gy'), may hold values from -6 to 6
- response: float32 [45], replicated, may hold values from 0.2 to 2
- basis: float32 [362, 45], replicated, may hold values from -0.875 to 0.875
- mask: int32 [32, 64, 128], P('gx', 'gy'), may hold values 0 or 1
- coefficients: float32 [45, 32, 64, 128], P(None, 'gx', 'gy'), may hold values from -6 to 6
- extrapolated: float32 [45, 32, 64, 128], P(None, 'gx', 'gy'), may hold values from -6 to 6
- dual_grad: float32 [3, 362, 32, 64, 128], P(None, None, 'gx', 'gy'), may hold values from -2 to 2
- dual_sign: float32 [362, 32, 64, 128], P(None, 'gx', 'gy'), may hold values from -1 to 0
Outputs:
- coefficients_out: float32 [45, 32, 64, 128], P(None, 'gx', 'gy')
- extrapolated_out: float32 [45, 32, 64, 128], P(None, 'gx', 'gy')
- dual_grad_out: float32 [3, 362, 32, 64, 128], P(None, None, 'gx', 'gy')
- dual_sign_out: float32 [362, 32, 64, 128], P(None, 'gx', 'gy')
The draws below stay inside these ranges and needn't reach their ends.
Inputs may be any that keep to these rules, and one draw needn't show every extreme that they name: `mask`: 1 marks a voxel inside the brain.
All inputs are finite; a program needn't handle non-finite values. No bound on the sum of `mask` on one device may be relied on, other than what follows from the above.
Results may differ from the reference program's by a relative error of at most 0.0001.
Values sent between devices are 32-bit elements; how exact they have to be, the bound alone decides.
A program may use at most 64 MiB of HBM per device.

```python
import math
import jax
import jax.numpy as jnp
from jax import lax

NCOEF = 45
NDIR = 362
PLANES = 128
ITERS = 2
NX = 32
NY = 64


def set_ends(entries, stream_key, smallest, largest):
    index_at = [jax.random.randint(jax.random.fold_in(stream_key, axis), (), 0, length) for axis, length in enumerate(entries.shape)]
    longest = entries.shape.index(max(entries.shape))
    beside = index_at[:longest] + [(index_at[longest] + 1) % entries.shape[longest]] + index_at[longest + 1:]
    return entries.at[tuple(index_at)].set(smallest).at[tuple(beside)].set(largest)


def block_scale(rng, extent, split, least, high):
    gain = 1.0
    for axis_at, shards_of in split:
        draws = jax.random.uniform(jax.random.fold_in(jax.random.fold_in(rng, 6), axis_at), (shards_of,), jnp.float32, least / len(split), high / len(split))
        gain = gain * jnp.repeat(jnp.exp(draws), extent[axis_at] // shards_of).reshape((-1,) + (1,) * (len(extent) - 1 - axis_at))
    return gain


def noise(stream_key, shape, width, bound, pieces=(), held_as=jnp.bfloat16):
    level = block_scale(stream_key, shape, pieces, -0.22, 0.18) if pieces else 1.0
    array = jax.random.normal(stream_key, shape, jnp.float32) * width * level
    return jnp.minimum(jnp.maximum(array, -bound), bound).astype(held_as)


def setup_inputs(seed: int = 0) -> dict:
    seeds = jax.random.split(jax.random.key(seed), 9)
    signal = noise(seeds[0], (NCOEF, NX, NY, PLANES), 1.0, 6.0, ((1, 32), (2, 8)), jnp.float32)
    response = jnp.clip(jnp.exp(jax.random.uniform(seeds[1], (NCOEF,), jnp.float32, math.log(0.2), math.log(2.0))), 0.2, 2.0)
    basis = noise(seeds[2], (NDIR, NCOEF), NCOEF ** -0.5, 0.875, (), jnp.float32)
    mask = set_ends((jax.random.randint(seeds[3], (NX, NY, PLANES), 0, 4) < 3).astype(jnp.int32), jax.random.fold_in(seeds[3], 1), 0, 1)
    coefficients = noise(seeds[4], (NCOEF, NX, NY, PLANES), 1.0, 6.0, ((1, 32), (2, 8)), jnp.float32)
    extrapolated = noise(seeds[5], (NCOEF, NX, NY, PLANES), 1.0, 6.0, ((1, 32), (2, 8)), jnp.float32)
    dual_grad = noise(seeds[6], (3, NDIR, NX, NY, PLANES), 0.3, 2.0, ((2, 32), (3, 8)), jnp.float32)
    dual_sign = jnp.clip(-1.0 + 1.0 * jax.random.uniform(seeds[7], (NDIR, NX, NY, PLANES), jnp.float32) ** block_scale(seeds[7], (NDIR, NX, NY, PLANES), ((1, 32), (2, 8)), -0.2, 0.2), -1.0, 0.0)
    return {"signal": signal, "response": response, "basis": basis, "mask": mask, "coefficients": coefficients, "extrapolated": extrapolated, "dual_grad": dual_grad, "dual_sign": dual_sign}


STEP_PRIMAL = 0.25
STEP_DUAL = 0.02
TV_WEIGHT = 0.5

def to_sphere(basis, coef_rows):
    count = coef_rows.shape[0]
    result = jnp.dot(basis, coef_rows.reshape(count, -1), precision=lax.Precision.HIGHEST, preferred_element_type=jnp.float32)
    return result.reshape((basis.shape[0],) + coef_rows.shape[1:])

def to_harmonics(basis, amp_rows):
    count = amp_rows.shape[0]
    result = jnp.dot(basis.T, amp_rows.reshape(count, -1), precision=lax.Precision.HIGHEST, preferred_element_type=jnp.float32)
    return result.reshape((basis.shape[1],) + amp_rows.shape[1:])

def forward_diff(field, along):
    length = field.shape[along]
    upper_part = lax.slice_in_dim(field, 1, length, axis=along)
    lower_part = lax.slice_in_dim(field, 0, length - 1, axis=along)
    zero_face = jnp.zeros_like(lax.slice_in_dim(field, 0, 1, axis=along))
    return jnp.concatenate([upper_part - lower_part, zero_face], along)

def backward_diff(dual_part, along):
    length = dual_part.shape[along]
    kept_rows = lax.slice_in_dim(dual_part, 0, length - 1, axis=along)
    zero_face = jnp.zeros_like(lax.slice_in_dim(dual_part, 0, 1, axis=along))
    masked = jnp.concatenate([kept_rows, zero_face], along)
    before = jnp.concatenate([zero_face, kept_rows], along)
    return masked - before

def reference(signal, response, basis, mask, coefficients, extrapolated, dual_grad, dual_sign):
    weight = mask.astype(jnp.float32)[None] * response[:, None, None, None]
    target = STEP_PRIMAL * weight * signal
    divisor = 1.0 + STEP_PRIMAL * weight * response[:, None, None, None]
    for iteration in range(ITERS):
        sphere_now = to_sphere(basis, extrapolated)
        stepped = [dual_grad[spatial] + STEP_DUAL * forward_diff(sphere_now, spatial + 1) for spatial in range(3)]
        magnitude = jnp.sqrt(stepped[0] * stepped[0] + stepped[1] * stepped[1] + stepped[2] * stepped[2])
        shrink = jnp.maximum(1.0, magnitude / TV_WEIGHT)
        dual_grad = jnp.stack([part / shrink for part in stepped])
        dual_sign = jnp.minimum(0.0, dual_sign + STEP_DUAL * sphere_now)
        backward = dual_sign - (backward_diff(dual_grad[0], 1) + backward_diff(dual_grad[1], 2) + backward_diff(dual_grad[2], 3))
        trial_step = coefficients - STEP_PRIMAL * to_harmonics(basis, backward)
        updated = (trial_step + target) / divisor
        extrapolated = 2.0 * updated - coefficients
        coefficients = updated
    return (coefficients, extrapolated, dual_grad, dual_sign)
```

```python
import jax
import jax.numpy as jnp
from jax import lax
from jax.experimental import pallas as pl
from jax.experimental.pallas import tpu as pltpu
from jax.sharding import PartitionSpec as P

STEP_PRIMAL = 0.25
STEP_DUAL = 0.02
TV_WEIGHT = 0.5

C, CP = 45, 48
N, NP = 362, 368
Y, Z = 8, 128
F32, BF16 = jnp.float32, jnp.bfloat16
MESH = pl.DeviceIdType.MESH
HBM = pl.BlockSpec(memory_space=pltpu.HBM)
VM = pl.BlockSpec(memory_space=pltpu.VMEM)


def halves(value):
    high = value.astype(BF16)
    return high, (value - high.astype(F32)).astype(BF16)


def main_kernel(sig, resp, bas, mask, coef, ext, dg, ds,
                dual, cout, eout,
                own, ex, ey, cur, sg, tgt, rdiv, rdx, rdy, up,
                mown, mx, my, bas_v, resp_v, fwd_w, bwd_w, q, r,
                ep_s, hx_s, hy_s, ep_r, hx_r, epy_r, hxd_r, hyd_r, hy_r, hx2_s, hy2_s, hx2_r, hy2_r,
                load_sem, dual_sem, a_s, a_r, b_s, b_r, f_s, f_r):
    gx, gy = lax.axis_index("gx"), lax.axis_index("gy")
    nx, ny = lax.axis_size("gx"), lax.axis_size("gy")
    xp, xm = lax.rem(gx + 1, nx), lax.rem(gx + nx - 1, nx)
    yp, ym = lax.rem(gy + 1, ny), lax.rem(gy + ny - 1, ny)
    keep_x = jnp.where(gx == nx - 1, 0.0, 1.0).astype(F32)
    keep_y = jnp.where(gy == ny - 1, 0.0, 1.0).astype(F32)

    barrier = pltpu.get_barrier_semaphore()
    for where in ((xm, gy), (xp, gy), (gx, ym), (gx, yp), (xm, yp), (xp, ym)):
        pl.semaphore_signal(barrier, inc=1, device_id=where, device_id_type=MESH)

    def rows_in(src, dst, base):
        return [pltpu.make_async_copy(src.at[:, y, :], dst.at[y, pl.ds(0, C), :], load_sem.at[base + y]) for y in range(Y)]
    ext_in = rows_in(ext, own, 0)
    cur_in = rows_in(coef, cur, 8)
    sig_in = rows_in(sig, sg, 16)
    bas_in = pltpu.make_async_copy(bas, bas_v, load_sem.at[24])
    resp_in = pltpu.make_async_copy(resp, resp_v, load_sem.at[25])
    mask_in = pltpu.make_async_copy(mask, mown, load_sem.at[26])
    dual_in = [[pltpu.make_async_copy((dg.at[a] if a < 3 else ds).at[:, y, :], dual.at[a, y, pl.ds(0, N), :], dual_sem.at[y, a])
                for a in range(4)] for y in range(Y)]
    for copy in ext_in + [mask_in, bas_in, resp_in]:
        copy.start()
    for copy in cur_in + sig_in:
        copy.start()
    for y in range(Y):
        for copy in dual_in[y]:
            copy.start()

    bas_in.wait()
    b_hi, b_lo = halves(bas_v[...])
    k_at = lax.broadcasted_iota(jnp.int32, (C, 256), 0)
    l_at = lax.broadcasted_iota(jnp.int32, (C, 256), 1)
    sel_hi = jnp.where((l_at == k_at) | (l_at == k_at + CP), 1.0, 0.0).astype(BF16)
    sel_lo = jnp.where(l_at == k_at + 2 * CP, 1.0, 0.0).astype(BF16)
    turn = (((0,), (0,)), ((), ()))
    fwd_w[...] = jnp.zeros((NP, 256), BF16)
    fwd_w[0:N, :] = (lax.dot_general(b_hi, sel_hi, turn, preferred_element_type=F32)
                     + lax.dot_general(b_lo, sel_lo, turn, preferred_element_type=F32)).astype(BF16)
    bwd_w[...] = jnp.zeros((2 * CP, 768), BF16)
    bwd_w[0:C, 0:N] = b_hi
    bwd_w[0:C, NP:NP + N] = b_hi
    bwd_w[CP:CP + C, 0:N] = b_lo
    q[:, 3 * CP:256, :] = jnp.zeros((2, 256 - 3 * CP, 4 * Z), BF16)
    r[:, 2 * NP:768, :] = jnp.zeros((2, 768 - 2 * NP, 2 * Z), BF16)
    for a in range(4):
        for y in range(Y):
            dual[a, y, pl.ds(N, NP - N), :] = jnp.zeros((NP - N, Z), F32)
    resp_in.wait()
    eye_f = lax.broadcasted_iota(jnp.int32, (CP, C), 0) == lax.broadcasted_iota(jnp.int32, (CP, C), 1)
    resp_c = jnp.sum(jnp.where(eye_f, jnp.broadcast_to(resp_v[...], (CP, C)), 0.0), axis=1, keepdims=True)

    mask_in.wait()
    for copy in ext_in:
        copy.wait()
    pl.semaphore_wait(barrier, 6)

    def send(src, dst, sems, at, where):
        copy = pltpu.make_async_remote_copy(src_ref=src, dst_ref=dst, send_sem=sems[0].at[at], recv_sem=sems[1].at[at],
                                            device_id=where, device_id_type=MESH)
        copy.start()
        return copy
    real = pl.ds(0, C)
    ab = (a_s, a_r)
    sent_a = {"ey": send(own.at[0, real, :], ey.at[real, :], ab, 8, (gx, ym))}
    for y in range(Y):
        sent_a[y] = send(own.at[y, real, :], ex.at[y, real, :], ab, y, (xm, gy))
    sent_a["my"] = send(mown, my, ab, 9, (gx, ym))
    sent_a["mx"] = send(mown, mx, ab, 10, (xm, gy))

    def recip(mask_row):
        m = jnp.broadcast_to(mask_row.astype(F32), (CP, Z))
        w = m * resp_c
        return 1.0 / (1.0 + STEP_PRIMAL * w * resp_c), w
    for y in range(Y):
        sig_in[y].wait()
        cur_in[y].wait()
        inv, w = recip(mown[y:y + 1, :])
        rdiv[y] = inv
        tgt[y] = STEP_PRIMAL * w * sg[y]

    pad_ok = lax.broadcasted_iota(jnp.int32, (CP, Z), 0) < C
    lane_last = lax.broadcasted_iota(jnp.int32, (1, Z), 1) == Z - 1
    z_keep = jnp.where(lane_last, 0.0, 1.0).astype(F32)

    def forward(y):
        slot = y % 2
        here = own[y]
        if y < Y - 1:
            dy = (own[y + 1] - here) * STEP_DUAL
        else:
            dy = (ey[...] - here) * (STEP_DUAL * keep_y)
        dx = (ex[y] - here) * (STEP_DUAL * keep_x)
        dz = (pltpu.roll(here, Z - 1, 1) - here) * (STEP_DUAL * z_keep)
        for a, field in enumerate((dx, dy, dz, here * STEP_DUAL)):
            hi, lo = halves(jnp.where(pad_ok, field, 0.0))
            at = slice(a * Z, (a + 1) * Z)
            q[slot, 0:CP, at] = hi
            q[slot, CP:2 * CP, at] = lo
            q[slot, 2 * CP:3 * CP, at] = hi
        mm = jnp.dot(fwd_w[...], q[slot], preferred_element_type=F32)
        sx = dual[0, y] + mm[:, 0:Z]
        sy = dual[1, y] + mm[:, Z:2 * Z]
        sz = dual[2, y] + mm[:, 2 * Z:3 * Z]
        scale = jnp.minimum(1.0, TV_WEIGHT * lax.rsqrt(sx * sx + sy * sy + sz * sz))
        dual[0, y] = sx * scale
        dual[1, y] = sy * scale
        dual[2, y] = sz * scale
        dual[3, y] = jnp.minimum(0.0, dual[3, y] + mm[:, 3 * Z:4 * Z])

    def project(slot, last_values):
        res = jnp.dot(bwd_w[...], r[slot], preferred_element_type=F32)
        return res[0:CP] + res[CP:2 * CP]

    def backward(y):
        slot = y % 2
        across = dual[1, y]
        if y == Y - 1:
            across = across * keep_y
        deep = dual[2, y] * z_keep
        w = dual[3, y] - across - deep + pltpu.roll(deep, 1, 1)
        if y > 0:
            w = w + dual[1, y - 1]
        for a, field in enumerate((w, dual[0, y])):
            hi, lo = halves(field)
            r[slot, 0:NP, a * Z:(a + 1) * Z] = hi
            r[slot, NP:2 * NP, a * Z:(a + 1) * Z] = lo
        res = project(slot, None)
        hx = res[:, Z:2 * Z] * keep_x
        harm = res[:, 0:Z] - hx
        return hx, (cur[y] - STEP_PRIMAL * harm + tgt[y]) * rdiv[y]

    def face_y():
        hi, lo = halves(dual[1, Y - 1])
        r[0, 0:NP, 0:Z] = hi
        r[0, NP:2 * NP, 0:Z] = lo
        return project(0, None)[:, 0:Z] * keep_y

    bb = (b_s, b_r)
    sent_b = {}
    for y in range(Y):
        if y == Y - 1:
            sent_a["ey"].wait_recv()
        sent_a[y].wait_recv()
        for copy in dual_in[y]:
            copy.wait()
        forward(y)
        if y == Y - 1:
            hy_s[...] = face_y()
            sent_b["hy"] = send(hy_s.at[real, :], hy_r.at[real, :], bb, 16, (gx, yp))
            sent_b["hyd"] = send(hy_s.at[real, :], hyd_r.at[real, :], bb, 17, (xm, yp))
        hx, u = backward(y)
        hx_s[y] = hx
        up[y] = u
        ep_s[y] = 2.0 * u - cur[y]
        if y == 0:
            sent_b["epy"] = send(ep_s.at[0, real, :], epy_r.at[real, :], bb, 18, (gx, ym))
            sent_b["hxd"] = send(hx_s.at[0, real, :], hxd_r.at[real, :], bb, 19, (xp, ym))
        sent_b["hx", y] = send(hx_s.at[y, real, :], hx_r.at[y, real, :], bb, y, (xp, gy))
        sent_b["ep", y] = send(ep_s.at[y, real, :], ep_r.at[y, real, :], bb, 8 + y, (xm, gy))

    sent_a["mx"].wait_recv()
    sent_a["my"].wait_recv()
    for y in range(Y):
        rdx[y] = recip(mx[y:y + 1, :])[0]
    rdy[...] = recip(my[0:1, :])[0]
    for key in sent_a:
        sent_a[key].wait_send()

    def finish(y):
        sent_b["hx", y].wait_recv()
        sent_b["ep", y].wait_recv()
        face = hx_r[y]
        above = hx_s[y]
        if y == 0:
            sent_b["hy"].wait_recv()
            sent_b["hyd"].wait_recv()
            face = face + hy_r[...]
            above = above + hyd_r[...]
        c_new = up[y] - STEP_PRIMAL * rdiv[y] * face
        own[y] = 2.0 * c_new - cur[y]
        cur[y] = c_new
        ex[y] = ep_r[y] - 2.0 * STEP_PRIMAL * rdx[y] * above

    ff = (f_s, f_r)
    sent_f = {}

    def second_back(y):
        hx, u = backward(y)
        hx2_s[y] = hx
        up[y] = u
        sent_f["hx", y] = send(hx2_s.at[y, real, :], hx2_r.at[y, real, :], ff, y, (xp, gy))

    finish(1)
    for y in range(1, Y):
        if y < Y - 1:
            finish(y + 1)
        else:
            sent_b["epy"].wait_recv()
            sent_b["hxd"].wait_recv()
            ey[...] = epy_r[...] - 2.0 * STEP_PRIMAL * rdy[...] * (hy_s[...] + hxd_r[...])
        forward(y)
        if y == Y - 1:
            hy2_s[...] = face_y()
            sent_f["hy"] = send(hy2_s.at[real, :], hy2_r.at[real, :], ff, 8, (gx, yp))
        if y > 1:
            second_back(y)
    finish(0)
    forward(0)
    second_back(0)
    second_back(1)
    for key in sent_b:
        sent_b[key].wait_send()

    for y in (2, 3, 4, 5, 6, 7, 0, 1):
        sent_f["hx", y].wait_recv()
        face = hx2_r[y]
        if y == 0:
            sent_f["hy"].wait_recv()
            face = face + hy2_r[...]
        c_new = up[y] - STEP_PRIMAL * rdiv[y] * face
        cout[y] = c_new
        eout[y] = 2.0 * c_new - cur[y]
    for key in sent_f:
        sent_f[key].wait_send()


def write_kernel(dual, cnew, enew, c_o, e_o, dg_o, ds_o, sem):
    copies = []
    for y in range(Y):
        for a in range(4):
            dst = dg_o.at[a] if a < 3 else ds_o
            copies.append((dual.at[a, y, pl.ds(0, N), :], dst.at[:, y, :]))
        copies.append((cnew.at[y, pl.ds(0, C), :], c_o.at[:, y, :]))
        copies.append((enew.at[y, pl.ds(0, C), :], e_o.at[:, y, :]))
    copies = [pltpu.make_async_copy(src, dst, sem.at[i]) for i, (src, dst) in enumerate(copies)]
    for copy in copies:
        copy.start()
    for copy in copies:
        copy.wait()


def per_device(signal, response, basis, mask, coefficients, extrapolated, dual_grad, dual_sign):
    block = pltpu.VMEM((Y, CP, Z), F32)
    face = pltpu.VMEM((CP, Z), F32)
    dma = pltpu.SemaphoreType.DMA
    dual, cnew, enew = pl.pallas_call(
        main_kernel,
        out_shape=(pltpu.VMEM((4, Y, NP, Z), F32), pltpu.VMEM((Y, CP, Z), F32), pltpu.VMEM((Y, CP, Z), F32)),
        in_specs=[HBM] * 8,
        out_specs=(VM, VM, VM),
        scratch_shapes=[
            block, block, face, block, block, block, block, block, face, block,
            pltpu.VMEM((Y, Z), jnp.int32), pltpu.VMEM((Y, Z), jnp.int32), pltpu.VMEM((Y, Z), jnp.int32),
            pltpu.VMEM((C, N), F32), pltpu.VMEM((1, C), F32),
            pltpu.VMEM((NP, 256), BF16), pltpu.VMEM((2 * CP, 768), BF16),
            pltpu.VMEM((2, 256, 4 * Z), BF16), pltpu.VMEM((2, 768, 2 * Z), BF16),
            block, block, face, block, block, face, face, face, face, block, face, block, face,
            dma((27,)), dma((Y, 4)), dma((11,)), dma((11,)), dma((20,)), dma((20,)), dma((9,)), dma((9,)),
        ],
        compiler_params=pltpu.CompilerParams(collective_id=0, has_side_effects=True, vmem_limit_bytes=40 * 2**20),
        name="steps",
    )(*(pltpu.with_memory_space_constraint(value, pltpu.HBM) for value in (
        signal.reshape(C, Y, Z), response.reshape(1, C), basis.T, mask.reshape(Y, Z), coefficients.reshape(C, Y, Z),
        extrapolated.reshape(C, Y, Z), dual_grad.reshape(3, N, Y, Z), dual_sign.reshape(N, Y, Z),
    )))
    c_o, e_o, dg_o, ds_o = pl.pallas_call(
        write_kernel,
        out_shape=(jax.ShapeDtypeStruct((C, Y, Z), F32), jax.ShapeDtypeStruct((C, Y, Z), F32),
                   jax.ShapeDtypeStruct((3, N, Y, Z), F32), jax.ShapeDtypeStruct((N, Y, Z), F32)),
        in_specs=[VM] * 3,
        out_specs=(HBM,) * 4,
        scratch_shapes=[dma((6 * Y,))],
        compiler_params=pltpu.CompilerParams(vmem_limit_bytes=16 * 2**20),
        name="write",
    )(*(pltpu.with_memory_space_constraint(value, pltpu.VMEM) for value in (dual, cnew, enew)))
    return (c_o.reshape(coefficients.shape), e_o.reshape(coefficients.shape),
            dg_o.reshape(dual_grad.shape), ds_o.reshape(dual_sign.shape))


def solution(mesh):
    in_specs = (
        P(None, "gx", "gy", None), P(), P(), P("gx", "gy", None), P(None, "gx", "gy", None),
        P(None, "gx", "gy", None), P(None, None, "gx", "gy", None), P(None, "gx", "gy", None),
    )
    out_specs = (
        P(None, "gx", "gy", None), P(None, "gx", "gy", None), P(None, None, "gx", "gy", None), P(None, "gx", "gy", None),
    )
    return jax.shard_map(per_device, mesh=mesh, in_specs=in_specs, out_specs=out_specs, check_vma=False)
```

```python
import jax
import jax.numpy as jnp
from jax import lax
from jax.experimental import pallas as pl
from jax.experimental.pallas import tpu as pltpu
from jax.sharding import PartitionSpec as P

STEP_PRIMAL = 0.25
STEP_DUAL = 0.02
TV_WEIGHT = 0.5

C, CP = 45, 48
N, NP = 362, 368
Y, Z = 8, 128
F32, BF16 = jnp.float32, jnp.bfloat16
MESH = pl.DeviceIdType.MESH
HBM = pl.BlockSpec(memory_space=pltpu.HBM)
VM = pl.BlockSpec(memory_space=pltpu.VMEM)


def halves(value):
    high = value.astype(BF16)
    return high, (value - high.astype(F32)).astype(BF16)


def main_kernel(sig, resp, bas, mask, coef, ext, dg, ds,
                dual, cout, eout,
                own, ex, ey, cur, sg, tgt, rdiv, rdx, rdy, up,
                mown, mx, my, bas_v, resp_v, fwd_w, bwd_w, q, r,
                ep_s, hx_s, hy_s, ep_r, hx_r, epy_r, hxd_r, hyd_r, hy_r, hx2_s, hy2_s, hx2_r, hy2_r,
                load_sem, dual_sem, a_s, a_r, b_s, b_r, f_s, f_r):
    gx, gy = lax.axis_index("gx"), lax.axis_index("gy")
    nx, ny = lax.axis_size("gx"), lax.axis_size("gy")
    has_xp, has_xm, has_yp, has_ym = gx < nx - 1, gx > 0, gy < ny - 1, gy > 0
    to_xp, to_xm, to_yp, to_ym = (gx + 1, gy), (gx - 1, gy), (gx, gy + 1), (gx, gy - 1)
    up_left, down_right = (gx - 1, gy + 1), (gx + 1, gy - 1)
    has_ul, has_dr = jnp.logical_and(has_xm, has_yp), jnp.logical_and(has_xp, has_ym)
    keep_x = jnp.where(has_xp, 1.0, 0.0).astype(F32)
    keep_y = jnp.where(has_yp, 1.0, 0.0).astype(F32)

    barrier = pltpu.get_barrier_semaphore()

    @pl.when(has_xp)
    def _():
        pl.semaphore_signal(barrier, inc=1, device_id=to_xp, device_id_type=MESH)

    @pl.when(has_yp)
    def _():
        pl.semaphore_signal(barrier, inc=1, device_id=to_yp, device_id_type=MESH)

    def rows_in(src, dst, base):
        return [pltpu.make_async_copy(src.at[:, y, :], dst.at[y, pl.ds(0, C), :], load_sem.at[base + y]) for y in range(Y)]
    ext_in = rows_in(ext, own, 0)
    cur_in = rows_in(coef, cur, 8)
    sig_in = rows_in(sig, sg, 16)
    bas_in = pltpu.make_async_copy(bas, bas_v, load_sem.at[24])
    resp_in = pltpu.make_async_copy(resp, resp_v, load_sem.at[25])
    mask_in = pltpu.make_async_copy(mask, mown, load_sem.at[26])
    dual_in = [[pltpu.make_async_copy((dg.at[a] if a < 3 else ds).at[:, y, :], dual.at[a, y, pl.ds(0, N), :], dual_sem.at[y, a])
                for a in range(4)] for y in range(Y)]
    for copy in ext_in + [mask_in, bas_in, resp_in]:
        copy.start()
    for copy in cur_in + sig_in:
        copy.start()
    for y in range(Y):
        for copy in dual_in[y]:
            copy.start()

    zeros, face0 = jnp.zeros((Y, CP, Z), F32), jnp.zeros((CP, Z), F32)

    @pl.when(jnp.logical_not(has_xp))
    def _():
        ex[...] = zeros
        ep_r[...] = zeros
        mx[...] = jnp.zeros((Y, Z), jnp.int32)

    @pl.when(jnp.logical_not(has_xm))
    def _():
        hx_r[...] = zeros
        hx2_r[...] = zeros

    @pl.when(jnp.logical_not(has_yp))
    def _():
        ey[...] = face0
        epy_r[...] = face0
        my[...] = jnp.zeros((Y, Z), jnp.int32)

    @pl.when(jnp.logical_not(has_ym))
    def _():
        hy_r[...] = face0
        hy2_r[...] = face0

    @pl.when(jnp.logical_not(has_ul))
    def _():
        hxd_r[...] = face0

    @pl.when(jnp.logical_not(has_dr))
    def _():
        hyd_r[...] = face0

    bas_in.wait()
    b_hi, b_lo = halves(bas_v[...])
    k_at = lax.broadcasted_iota(jnp.int32, (C, 256), 0)
    l_at = lax.broadcasted_iota(jnp.int32, (C, 256), 1)
    sel_hi = jnp.where((l_at == k_at) | (l_at == k_at + CP), 1.0, 0.0).astype(BF16)
    sel_lo = jnp.where(l_at == k_at + 2 * CP, 1.0, 0.0).astype(BF16)
    turn = (((0,), (0,)), ((), ()))
    fwd_w[...] = jnp.zeros((NP, 256), BF16)
    fwd_w[0:N, :] = (lax.dot_general(b_hi, sel_hi, turn, preferred_element_type=F32)
                     + lax.dot_general(b_lo, sel_lo, turn, preferred_element_type=F32)).astype(BF16)
    bwd_w[...] = jnp.zeros((2 * CP, 768), BF16)
    bwd_w[0:C, 0:N] = b_hi
    bwd_w[0:C, NP:NP + N] = b_hi
    bwd_w[CP:CP + C, 0:N] = b_lo
    q[:, 3 * CP:256, :] = jnp.zeros((2, 256 - 3 * CP, 4 * Z), BF16)
    r[:, 2 * NP:768, :] = jnp.zeros((2, 768 - 2 * NP, 2 * Z), BF16)
    for a in range(4):
        for y in range(Y):
            dual[a, y, pl.ds(N, NP - N), :] = jnp.zeros((NP - N, Z), F32)
    resp_in.wait()
    eye_f = lax.broadcasted_iota(jnp.int32, (CP, C), 0) == lax.broadcasted_iota(jnp.int32, (CP, C), 1)
    resp_c = jnp.sum(jnp.where(eye_f, jnp.broadcast_to(resp_v[...], (CP, C)), 0.0), axis=1, keepdims=True)

    mask_in.wait()
    for copy in ext_in:
        copy.wait()

    @pl.when(jnp.logical_or(has_xm, has_ym))
    def _():
        pl.semaphore_wait(barrier, jnp.minimum(gx, 1) + jnp.minimum(gy, 1))

    class Message:
        def __init__(self, src, dst, sems, at, where, goes, comes):
            self.goes, self.comes = goes, comes
            self.copy = pltpu.make_async_remote_copy(src_ref=src, dst_ref=dst, send_sem=sems[0].at[at], recv_sem=sems[1].at[at],
                                                     device_id=where, device_id_type=MESH)
            pl.when(goes)(self.copy.start)

        def arrived(self):
            pl.when(self.comes)(self.copy.wait_recv)

        def left(self):
            pl.when(self.goes)(self.copy.wait_send)

    real = pl.ds(0, C)
    ab = (a_s, a_r)
    sent_a = {"ey": Message(own.at[0, real, :], ey.at[real, :], ab, 4, to_ym, has_ym, has_yp)}
    for p in range(4):
        two = pl.ds(2 * p, 2)
        sent_a[p] = Message(own.at[two, real, :], ex.at[two, real, :], ab, p, to_xm, has_xm, has_xp)
    sent_a["my"] = Message(mown, my, ab, 5, to_ym, has_ym, has_yp)
    sent_a["mx"] = Message(mown, mx, ab, 6, to_xm, has_xm, has_xp)

    def recip(mask_row):
        m = jnp.broadcast_to(mask_row.astype(F32), (CP, Z))
        w = m * resp_c
        return 1.0 / (1.0 + STEP_PRIMAL * w * resp_c), w
    for copy in sig_in + cur_in:
        copy.wait()
    for y in range(Y):
        inv, w = recip(mown[y:y + 1, :])
        rdiv[y] = inv
        tgt[y] = STEP_PRIMAL * w * sg[y]

    pad_ok = lax.broadcasted_iota(jnp.int32, (CP, Z), 0) < C
    lane_last = lax.broadcasted_iota(jnp.int32, (1, Z), 1) == Z - 1
    z_keep = jnp.where(lane_last, 0.0, 1.0).astype(F32)

    def lift(slot, fields):
        for a, field in enumerate(fields):
            hi, lo = halves(jnp.where(pad_ok, field, 0.0))
            at = slice(a * Z, (a + 1) * Z)
            q[slot, 0:CP, at] = hi
            q[slot, CP:2 * CP, at] = lo
            q[slot, 2 * CP:3 * CP, at] = hi
        mm = jnp.dot(fwd_w[...], q[slot, :, 0:len(fields) * Z], preferred_element_type=F32)
        return [mm[:, a * Z:(a + 1) * Z] for a in range(len(fields))]

    def diff_x(y):
        return (ex[y] - own[y]) * (STEP_DUAL * keep_x)

    def diff_y(y):
        if y < Y - 1:
            return (own[y + 1] - own[y]) * STEP_DUAL
        return (ey[...] - own[y]) * (STEP_DUAL * keep_y)

    def diff_z(y):
        return (pltpu.roll(own[y], Z - 1, 1) - own[y]) * (STEP_DUAL * z_keep)

    def shrink(y, sx, sy, sz):
        scale = jnp.minimum(1.0, TV_WEIGHT * lax.rsqrt(sx * sx + sy * sy + sz * sz))
        dual[0, y] = sx * scale
        dual[1, y] = sy * scale
        dual[2, y] = sz * scale

    def sign(y, amp):
        dual[3, y] = jnp.minimum(0.0, dual[3, y] + amp)

    def drop(slot, values):
        for a, value in enumerate(values):
            hi, lo = halves(value)
            r[slot, 0:NP, a * Z:(a + 1) * Z] = hi
            r[slot, NP:2 * NP, a * Z:(a + 1) * Z] = lo
        res = jnp.dot(bwd_w[...], r[slot, :, 0:len(values) * Z], preferred_element_type=F32)
        res = res[0:CP] + res[CP:2 * CP]
        return [res[:, a * Z:(a + 1) * Z] for a in range(len(values))]

    def inner(y):
        across = dual[1, y]
        if y == Y - 1:
            across = across * keep_y
        deep = dual[2, y] * z_keep
        w = dual[3, y] - across - deep + pltpu.roll(deep, 1, 1)
        if y > 0:
            w = w + dual[1, y - 1]
        return w

    def advance(y, harm):
        return (cur[y] - STEP_PRIMAL * harm + tgt[y]) * rdiv[y]

    for y in range(Y):
        for copy in dual_in[y]:
            copy.wait()
    for y in range(Y):
        fields = [diff_z(y), own[y] * STEP_DUAL]
        if y < Y - 1:
            fields.append(diff_y(y))
        mm = lift(y % 2, fields)
        dual[2, y] = dual[2, y] + mm[0]
        sign(y, mm[1])
        if y < Y - 1:
            dual[1, y] = dual[1, y] + mm[2]

    bb = (b_s, b_r)
    sent_b = {}
    for p in range(4):
        ya, yb = 2 * p, 2 * p + 1
        two = pl.ds(ya, 2)
        sent_a[p].arrived()
        if yb == Y - 1:
            sent_a["ey"].arrived()
            mm = lift(p % 2, [diff_x(yb), diff_y(yb), diff_x(ya)])
            shrink(yb, dual[0, yb] + mm[0], dual[1, yb] + mm[1], dual[2, yb])
            hy_s[...] = drop(0, [dual[1, yb]])[0] * keep_y
            sent_b["hy"] = Message(hy_s.at[real, :], hy_r.at[real, :], bb, 8, to_yp, has_yp, has_ym)
            sent_b["hyd"] = Message(hy_s.at[real, :], hyd_r.at[real, :], bb, 9, up_left, has_ul, has_dr)
            shrink(ya, dual[0, ya] + mm[2], dual[1, ya], dual[2, ya])
        else:
            mm = lift(p % 2, [diff_x(ya), diff_x(yb)])
            for y, part in ((ya, mm[0]), (yb, mm[1])):
                shrink(y, dual[0, y] + part, dual[1, y], dual[2, y])
        faces = drop(0, [dual[0, ya], dual[0, yb]])
        harms = drop(1, [inner(ya), inner(yb)])
        for y, face, harm in ((ya, faces[0], harms[0]), (yb, faces[1], harms[1])):
            face = face * keep_x
            hx_s[y] = face
            u = advance(y, harm - face)
            up[y] = u
            ep_s[y] = 2.0 * u - cur[y]
        if p == 0:
            sent_b["epy"] = Message(ep_s.at[0, real, :], epy_r.at[real, :], bb, 10, to_ym, has_ym, has_yp)
            sent_b["hxd"] = Message(hx_s.at[0, real, :], hxd_r.at[real, :], bb, 11, down_right, has_dr, has_ul)
        sent_b["hx", p] = Message(hx_s.at[two, real, :], hx_r.at[two, real, :], bb, p, to_xp, has_xp, has_xm)
        sent_b["ep", p] = Message(ep_s.at[two, real, :], ep_r.at[two, real, :], bb, 4 + p, to_xm, has_xm, has_xp)

    sent_a["mx"].arrived()
    sent_a["my"].arrived()
    for y in range(Y):
        rdx[y] = recip(mx[y:y + 1, :])[0]
    rdy[...] = recip(my[0:1, :])[0]
    for key in sent_a:
        sent_a[key].left()

    def pair_here(p):
        sent_b["hx", p].arrived()
        sent_b["ep", p].arrived()

    def finish(y):
        face = hx_r[y]
        above = hx_s[y]
        if y == 0:
            face = face + hy_r[...]
            above = above + hyd_r[...]
        c_new = up[y] - STEP_PRIMAL * rdiv[y] * face
        own[y] = 2.0 * c_new - cur[y]
        cur[y] = c_new
        ex[y] = ep_r[y] - 2.0 * STEP_PRIMAL * rdx[y] * above

    ff = (f_s, f_r)
    sent_f = {}

    def forward(y):
        mm = lift(y % 2, [diff_x(y), diff_y(y), diff_z(y), own[y] * STEP_DUAL])
        shrink(y, dual[0, y] + mm[0], dual[1, y] + mm[1], dual[2, y] + mm[2])
        sign(y, mm[3])

    def send_faces(rows):
        for y, face in zip(rows, drop(0, [dual[0, y] for y in rows])):
            hx2_s[y] = face * keep_x
        for y in rows:
            sent_f["hx", y] = Message(hx2_s.at[y, real, :], hx2_r.at[y, real, :], ff, y, to_xp, has_xp, has_xm)

    pair_here(0)
    pair_here(1)
    for y in (1, 2, 3):
        finish(y)
    forward(1)
    forward(2)
    send_faces((1, 2))
    pair_here(2)
    finish(4)
    finish(5)
    forward(3)
    forward(4)
    send_faces((3, 4))
    pair_here(3)
    sent_b["epy"].arrived()
    sent_b["hxd"].arrived()
    finish(6)
    finish(7)
    ey[...] = epy_r[...] - 2.0 * STEP_PRIMAL * rdy[...] * (hy_s[...] + hxd_r[...])
    forward(7)
    hy2_s[...] = drop(0, [dual[1, Y - 1]])[0] * keep_y
    sent_f["hy"] = Message(hy2_s.at[real, :], hy2_r.at[real, :], ff, 8, to_yp, has_yp, has_ym)
    forward(5)
    forward(6)
    send_faces((6, 7))
    send_faces((5,))
    sent_b["hy"].arrived()
    sent_b["hyd"].arrived()
    finish(0)
    forward(0)
    send_faces((0,))

    for p in range(4):
        ya, yb = 2 * p, 2 * p + 1
        harms = drop(p % 2, [inner(ya), inner(yb)])
        for y, harm in ((ya, harms[0]), (yb, harms[1])):
            up[y] = advance(y, harm - hx2_s[y])
    for key in sent_b:
        sent_b[key].left()

    for y in (1, 2, 3, 4, 6, 7, 5, 0):
        sent_f["hx", y].arrived()
        face = hx2_r[y]
        if y == 0:
            sent_f["hy"].arrived()
            face = face + hy2_r[...]
        c_new = up[y] - STEP_PRIMAL * rdiv[y] * face
        cout[y] = c_new
        eout[y] = 2.0 * c_new - cur[y]
    for key in sent_f:
        sent_f[key].left()


def write_kernel(dual, cnew, enew, c_o, e_o, dg_o, ds_o, sem):
    copies = []
    for y in range(Y):
        for a in range(4):
            dst = dg_o.at[a] if a < 3 else ds_o
            copies.append((dual.at[a, y, pl.ds(0, N), :], dst.at[:, y, :]))
        copies.append((cnew.at[y, pl.ds(0, C), :], c_o.at[:, y, :]))
        copies.append((enew.at[y, pl.ds(0, C), :], e_o.at[:, y, :]))
    copies = [pltpu.make_async_copy(src, dst, sem.at[i]) for i, (src, dst) in enumerate(copies)]
    for copy in copies:
        copy.start()
    for copy in copies:
        copy.wait()


def per_device(signal, response, basis, mask, coefficients, extrapolated, dual_grad, dual_sign):
    block = pltpu.VMEM((Y, CP, Z), F32)
    face = pltpu.VMEM((CP, Z), F32)
    dma = pltpu.SemaphoreType.DMA
    dual, cnew, enew = pl.pallas_call(
        main_kernel,
        out_shape=(pltpu.VMEM((4, Y, NP, Z), F32), pltpu.VMEM((Y, CP, Z), F32), pltpu.VMEM((Y, CP, Z), F32)),
        in_specs=[HBM] * 8,
        out_specs=(VM, VM, VM),
        scratch_shapes=[
            block, block, face, block, block, block, block, block, face, block,
            pltpu.VMEM((Y, Z), jnp.int32), pltpu.VMEM((Y, Z), jnp.int32), pltpu.VMEM((Y, Z), jnp.int32),
            pltpu.VMEM((C, N), F32), pltpu.VMEM((1, C), F32),
            pltpu.VMEM((NP, 256), BF16), pltpu.VMEM((2 * CP, 768), BF16),
            pltpu.VMEM((2, 256, 4 * Z), BF16), pltpu.VMEM((2, 768, 2 * Z), BF16),
            block, block, face, block, block, face, face, face, face, block, face, block, face,
            dma((27,)), dma((Y, 4)), dma((7,)), dma((7,)), dma((12,)), dma((12,)), dma((9,)), dma((9,)),
        ],
        compiler_params=pltpu.CompilerParams(collective_id=0, has_side_effects=True, vmem_limit_bytes=40 * 2**20),
        name="steps",
    )(*(pltpu.with_memory_space_constraint(value, pltpu.HBM) for value in (
        signal.reshape(C, Y, Z), response.reshape(1, C), basis.T, mask.reshape(Y, Z), coefficients.reshape(C, Y, Z),
        extrapolated.reshape(C, Y, Z), dual_grad.reshape(3, N, Y, Z), dual_sign.reshape(N, Y, Z),
    )))
    c_o, e_o, dg_o, ds_o = pl.pallas_call(
        write_kernel,
        out_shape=(jax.ShapeDtypeStruct((C, Y, Z), F32), jax.ShapeDtypeStruct((C, Y, Z), F32),
                   jax.ShapeDtypeStruct((3, N, Y, Z), F32), jax.ShapeDtypeStruct((N, Y, Z), F32)),
        in_specs=[VM] * 3,
        out_specs=(HBM,) * 4,
        scratch_shapes=[dma((6 * Y,))],
        compiler_params=pltpu.CompilerParams(vmem_limit_bytes=16 * 2**20),
        name="write",
    )(*(pltpu.with_memory_space_constraint(value, pltpu.VMEM) for value in (dual, cnew, enew)))
    return (c_o.reshape(coefficients.shape), e_o.reshape(coefficients.shape),
            dg_o.reshape(dual_grad.shape), ds_o.reshape(dual_sign.shape))


def solution(mesh):
    in_specs = (
        P(None, "gx", "gy", None), P(), P(), P("gx", "gy", None), P(None, "gx", "gy", None),
        P(None, "gx", "gy", None), P(None, None, "gx", "gy", None), P(None, "gx", "gy", None),
    )
    out_specs = (
        P(None, "gx", "gy", None), P(None, "gx", "gy", None), P(None, None, "gx", "gy", None), P(None, "gx", "gy", None),
    )
    return jax.shard_map(per_device, mesh=mesh, in_specs=in_specs, out_specs=out_specs, check_vma=False)
```

```python
import jax
import jax.numpy as jnp
from jax import lax
from jax.experimental import pallas as pl
from jax.experimental.pallas import tpu as pltpu
from jax.sharding import PartitionSpec as P

STEP_PRIMAL = 0.25
STEP_DUAL = 0.02
TV_WEIGHT = 0.5

C, CP = 45, 48
N, NP = 362, 368
Y, Z = 8, 128
F32, BF16 = jnp.float32, jnp.bfloat16
MESH = pl.DeviceIdType.MESH
HBM = pl.BlockSpec(memory_space=pltpu.HBM)
VM = pl.BlockSpec(memory_space=pltpu.VMEM)


def halves(value):
    high = value.astype(BF16)
    return high, (value - high.astype(F32)).astype(BF16)


def main_kernel(sig, resp, bas, mask, coef, ext, dg, ds,
                dual, cout, eout,
                own, ex, ey, cur, sg, tgt, rdiv, rdx, rdy, up,
                mown, mx, my, bas_v, resp_v, fwd_w, bwd_w, q, r,
                ep_s, hx_s, hy_s, ep_r, hx_r, epy_r, hxd_r, hyd_r, hy_r, hx2_s, hy2_s, hx2_r, hy2_r,
                load_sem, dual_sem, a_s, a_r, b_s, b_r, f_s, f_r, ready, ready_d):
    gx, gy = lax.axis_index("gx"), lax.axis_index("gy")
    nx, ny = lax.axis_size("gx"), lax.axis_size("gy")
    has_xp, has_xm, has_yp, has_ym = gx < nx - 1, gx > 0, gy < ny - 1, gy > 0
    to_xp, to_xm, to_yp, to_ym = (gx + 1, gy), (gx - 1, gy), (gx, gy + 1), (gx, gy - 1)
    up_left, down_right = (gx - 1, gy + 1), (gx + 1, gy - 1)
    has_ul, has_dr = jnp.logical_and(has_xm, has_yp), jnp.logical_and(has_xp, has_ym)
    far_above = jnp.logical_and(lax.rem(gx, 8) == 7, has_xp)
    far_below = jnp.logical_and(lax.rem(gx, 8) == 0, has_xm)
    keep_x = jnp.where(has_xp, 1.0, 0.0).astype(F32)
    keep_y = jnp.where(has_yp, 1.0, 0.0).astype(F32)

    odd = lax.rem(gy, 2) == 1
    even = jnp.logical_not(odd)
    head = lax.rem(gx, 8) == 0
    tail = jnp.logical_or(lax.rem(gx, 8) == 7, gx == nx - 1)
    barrier = pltpu.get_barrier_semaphore()

    def both(*flags):
        out = flags[0]
        for flag in flags[1:]:
            out = jnp.logical_and(out, flag)
        return out

    def greet(sem, when, where):
        @pl.when(when)
        def _():
            pl.semaphore_signal(sem, inc=1, device_id=where, device_id_type=MESH)

    greet(barrier, has_xp, to_xp)
    greet(barrier, both(even, has_yp), to_yp)
    greet(barrier, both(even, has_ym), to_ym)
    greet(barrier, both(even, has_dr), down_right)

    def rows_in(src, dst, base):
        return [pltpu.make_async_copy(src.at[:, y, :], dst.at[y, pl.ds(0, C), :], load_sem.at[base + y]) for y in range(Y)]
    ext_in = rows_in(ext, own, 0)
    cur_in = rows_in(coef, cur, 8)
    sig_in = rows_in(sig, sg, 16)
    bas_in = pltpu.make_async_copy(bas, bas_v, load_sem.at[24])
    resp_in = pltpu.make_async_copy(resp, resp_v, load_sem.at[25])
    mask_in = pltpu.make_async_copy(mask, mown, load_sem.at[26])
    dual_in = [[pltpu.make_async_copy((dg.at[a] if a < 3 else ds).at[:, y, :], dual.at[a, y, pl.ds(0, N), :], dual_sem.at[y, a])
                for a in range(4)] for y in range(Y)]
    for copy in ext_in + [mask_in, bas_in, resp_in]:
        copy.start()
    for copy in cur_in + sig_in:
        copy.start()
    for y in range(Y):
        for copy in dual_in[y]:
            copy.start()

    left, up_there = jnp.minimum(gx, 1), jnp.minimum(ny - 1 - gy, 1)

    @pl.when(jnp.logical_or(has_xm, odd))
    def _():
        pl.semaphore_wait(barrier, left + lax.rem(gy, 2) * (1 + up_there + left * up_there))

    greet(ready, both(odd, has_ul, jnp.logical_not(head)), up_left)
    greet(ready, both(odd, has_yp, tail), to_yp)
    greet(ready_d, both(odd, has_ul, head), up_left)

    for copy in ext_in:
        copy.wait()

    class Message:
        def __init__(self, src, dst, sems, at, where, goes, comes, now=True):
            self.goes, self.comes = goes, comes
            self.copy = pltpu.make_async_remote_copy(src_ref=src, dst_ref=dst, send_sem=sems[0].at[at], recv_sem=sems[1].at[at],
                                                     device_id=where, device_id_type=MESH)
            if now:
                self.go()

        def go(self):
            pl.when(self.goes)(self.copy.start)

        def arrived(self):
            pl.when(self.comes)(self.copy.wait_recv)

        def left(self):
            pl.when(self.goes)(self.copy.wait_send)

    real = pl.ds(0, C)
    ab = (a_s, a_r)
    sent_a = {}
    face_copy = pltpu.make_async_remote_copy(src_ref=own.at[0, real, :], dst_ref=ey.at[real, :], send_sem=a_s.at[4], recv_sem=a_r.at[4],
                                             device_id=to_ym, device_id_type=MESH)

    @pl.when(both(odd, has_ym))
    def _():
        face_copy.start()
    for p in (3, 0, 1, 2):
        two = pl.ds(2 * p, 2)
        sent_a[p] = Message(own.at[two, real, :], ex.at[two, real, :], ab, p, to_xm, has_xm, has_xp)

    zeros, face0 = jnp.zeros((Y, CP, Z), F32), jnp.zeros((CP, Z), F32)

    @pl.when(jnp.logical_not(has_xp))
    def _():
        ex[...] = zeros
        ep_r[...] = zeros
        mx[...] = jnp.zeros((Y, Z), jnp.int32)

    @pl.when(jnp.logical_not(has_xm))
    def _():
        hx_r[...] = zeros
        hx2_r[...] = zeros

    @pl.when(jnp.logical_not(has_yp))
    def _():
        ey[...] = face0
        epy_r[...] = face0
        my[...] = jnp.zeros((Y, Z), jnp.int32)

    @pl.when(jnp.logical_not(has_ym))
    def _():
        hy_r[...] = face0
        hy2_r[...] = face0

    @pl.when(jnp.logical_not(has_ul))
    def _():
        hxd_r[...] = face0

    @pl.when(jnp.logical_not(has_dr))
    def _():
        hyd_r[...] = face0

    bas_in.wait()
    b_hi, b_lo = halves(bas_v[...])
    k_at = lax.broadcasted_iota(jnp.int32, (C, 256), 0)
    l_at = lax.broadcasted_iota(jnp.int32, (C, 256), 1)
    sel_hi = jnp.where((l_at == k_at) | (l_at == k_at + CP), 1.0, 0.0).astype(BF16)
    sel_lo = jnp.where(l_at == k_at + 2 * CP, 1.0, 0.0).astype(BF16)
    turn = (((0,), (0,)), ((), ()))
    fwd_w[...] = jnp.zeros((NP, 256), BF16)
    fwd_w[0:N, :] = (lax.dot_general(b_hi, sel_hi, turn, preferred_element_type=F32)
                     + lax.dot_general(b_lo, sel_lo, turn, preferred_element_type=F32)).astype(BF16)
    bwd_w[...] = jnp.zeros((2 * CP, 768), BF16)
    bwd_w[0:C, 0:N] = b_hi
    bwd_w[0:C, NP:NP + N] = b_hi
    bwd_w[CP:CP + C, 0:N] = b_lo
    q[:, 3 * CP:256, :] = jnp.zeros((2, 256 - 3 * CP, 4 * Z), BF16)
    r[:, 2 * NP:768, :] = jnp.zeros((2, 768 - 2 * NP, 2 * Z), BF16)
    for a in range(4):
        for y in range(Y):
            dual[a, y, pl.ds(N, NP - N), :] = jnp.zeros((NP - N, Z), F32)
    resp_in.wait()
    eye_f = lax.broadcasted_iota(jnp.int32, (CP, C), 0) == lax.broadcasted_iota(jnp.int32, (CP, C), 1)
    resp_c = jnp.sum(jnp.where(eye_f, jnp.broadcast_to(resp_v[...], (CP, C)), 0.0), axis=1, keepdims=True)

    mask_in.wait()

    def recip(mask_row):
        m = jnp.broadcast_to(mask_row.astype(F32), (CP, Z))
        w = m * resp_c
        return 1.0 / (1.0 + STEP_PRIMAL * w * resp_c), w
    for copy in sig_in + cur_in:
        copy.wait()
    for y in range(Y):
        inv, w = recip(mown[y:y + 1, :])
        rdiv[y] = inv
        tgt[y] = STEP_PRIMAL * w * sg[y]

    pad_ok = lax.broadcasted_iota(jnp.int32, (CP, Z), 0) < C
    lane_last = lax.broadcasted_iota(jnp.int32, (1, Z), 1) == Z - 1
    z_keep = jnp.where(lane_last, 0.0, 1.0).astype(F32)

    def lift(slot, fields):
        for a, field in enumerate(fields):
            hi, lo = halves(jnp.where(pad_ok, field, 0.0))
            at = slice(a * Z, (a + 1) * Z)
            q[slot, 0:CP, at] = hi
            q[slot, CP:2 * CP, at] = lo
            q[slot, 2 * CP:3 * CP, at] = hi
        mm = jnp.dot(fwd_w[...], q[slot, :, 0:len(fields) * Z], preferred_element_type=F32)
        return [mm[:, a * Z:(a + 1) * Z] for a in range(len(fields))]

    def diff_x(y):
        return (ex[y] - own[y]) * (STEP_DUAL * keep_x)

    def diff_y(y):
        if y < Y - 1:
            return (own[y + 1] - own[y]) * STEP_DUAL
        return (ey[...] - own[y]) * (STEP_DUAL * keep_y)

    def diff_z(y):
        return (pltpu.roll(own[y], Z - 1, 1) - own[y]) * (STEP_DUAL * z_keep)

    def shrink(y, sx, sy, sz):
        scale = jnp.minimum(1.0, TV_WEIGHT * lax.rsqrt(sx * sx + sy * sy + sz * sz))
        dual[0, y] = sx * scale
        dual[1, y] = sy * scale
        dual[2, y] = sz * scale

    def sign(y, amp):
        dual[3, y] = jnp.minimum(0.0, dual[3, y] + amp)

    def drop(slot, values):
        for a, value in enumerate(values):
            hi, lo = halves(value)
            r[slot, 0:NP, a * Z:(a + 1) * Z] = hi
            r[slot, NP:2 * NP, a * Z:(a + 1) * Z] = lo
        res = jnp.dot(bwd_w[...], r[slot, :, 0:len(values) * Z], preferred_element_type=F32)
        res = res[0:CP] + res[CP:2 * CP]
        return [res[:, a * Z:(a + 1) * Z] for a in range(len(values))]

    def inner(y):
        across = dual[1, y]
        if y == Y - 1:
            across = across * keep_y
        deep = dual[2, y] * z_keep
        w = dual[3, y] - across - deep + pltpu.roll(deep, 1, 1)
        if y > 0:
            w = w + dual[1, y - 1]
        return w

    def advance(y, harm):
        return (cur[y] - STEP_PRIMAL * harm + tgt[y]) * rdiv[y]

    for y in range(Y):
        for copy in dual_in[y]:
            copy.wait()
    def alone(y):
        fields = [diff_z(y), own[y] * STEP_DUAL]
        if y < Y - 1:
            fields.append(diff_y(y))
        mm = lift(y % 2, fields)
        dual[2, y] = dual[2, y] + mm[0]
        sign(y, mm[1])
        if y < Y - 1:
            dual[1, y] = dual[1, y] + mm[2]
    for y in range(Y // 2):
        alone(y)

    @pl.when(both(even, has_ym))
    def _():
        pl.semaphore_wait(ready, 1)
        face_copy.start()
    sent_a["my"] = Message(mown, my, ab, 5, to_ym, has_ym, has_yp)
    sent_a["mx"] = Message(mown, mx, ab, 6, to_xm, has_xm, has_xp)
    for y in range(Y // 2, Y):
        alone(y)

    bb = (b_s, b_r)
    sent_b = {
        "hy": Message(hy_s.at[real, :], hy_r.at[real, :], bb, 8, to_yp, has_yp, has_ym, False),
        "hyd": Message(hy_s.at[real, :], hyd_r.at[real, :], bb, 9, up_left, has_ul, has_dr, False),
        "hx7": Message(hx_s.at[7, real, :], hx_r.at[7, real, :], bb, 12, to_xp, has_xp, has_xm, False),
    }

    def last_row():
        sent_a[3].arrived()
        pl.when(has_yp)(face_copy.wait_recv)
        mm = lift(1, [diff_x(7), diff_y(7)])
        shrink(7, dual[0, 7] + mm[0], dual[1, 7] + mm[1], dual[2, 7])
        across, face = drop(1, [dual[1, 7], dual[0, 7]])
        hy_s[...] = across * keep_y
        hx_s[7] = face * keep_x
        for key in ("hy", "hyd", "hx7"):
            sent_b[key].go()

    pl.when(far_above)(last_row)
    for p in range(4):
        ya, yb = 2 * p, 2 * p + 1
        two = pl.ds(ya, 2)
        if p == 3:
            pl.when(jnp.logical_not(far_above))(last_row)
            mm = lift(0, [diff_x(6)])
            shrink(6, dual[0, 6] + mm[0], dual[1, 6], dual[2, 6])
            hx_s[6] = drop(0, [dual[0, 6]])[0] * keep_x
        else:
            sent_a[p].arrived()
            mm = lift(0, [diff_x(ya), diff_x(yb)])
            for y, part in ((ya, mm[0]), (yb, mm[1])):
                shrink(y, dual[0, y] + part, dual[1, y], dual[2, y])
            for y, face in zip((ya, yb), drop(0, [dual[0, ya], dual[0, yb]])):
                hx_s[y] = face * keep_x
        for y, harm in zip((ya, yb), drop(1, [inner(ya), inner(yb)])):
            u = advance(y, harm - hx_s[y])
            up[y] = u
            ep_s[y] = 2.0 * u - cur[y]
        if p == 0:
            sent_b["epy"] = Message(ep_s.at[0, real, :], epy_r.at[real, :], bb, 10, to_ym, has_ym, has_yp)
            @pl.when(both(even, has_dr, tail))
            def _():
                pl.semaphore_wait(ready_d, 1)
            sent_b["hxd"] = Message(hx_s.at[0, real, :], hxd_r.at[real, :], bb, 11, down_right, has_dr, has_ul)
        if p < 3:
            sent_b["hx", p] = Message(hx_s.at[two, real, :], hx_r.at[two, real, :], bb, p, to_xp, has_xp, has_xm)
        else:
            sent_b["hx", p] = Message(hx_s.at[6, real, :], hx_r.at[6, real, :], bb, p, to_xp, has_xp, has_xm)
        sent_b["ep", p] = Message(ep_s.at[two, real, :], ep_r.at[two, real, :], bb, 4 + p, to_xm, has_xm, has_xp)

    sent_a["mx"].arrived()
    sent_a["my"].arrived()
    for y in range(Y):
        rdx[y] = recip(mx[y:y + 1, :])[0]
    rdy[...] = recip(my[0:1, :])[0]
    pl.when(has_ym)(face_copy.wait_send)
    for key in sent_a:
        sent_a[key].left()

    def pair_here(p):
        sent_b["hx", p].arrived()
        sent_b["ep", p].arrived()

    def finish(y):
        face = hx_r[y]
        above = hx_s[y]
        if y == 0:
            face = face + hy_r[...]
            above = above + hyd_r[...]
        c_new = up[y] - STEP_PRIMAL * rdiv[y] * face
        own[y] = 2.0 * c_new - cur[y]
        cur[y] = c_new
        ex[y] = ep_r[y] - 2.0 * STEP_PRIMAL * rdx[y] * above

    ff = (f_s, f_r)
    sent_f = {}

    def forward(y):
        mm = lift(y % 2, [diff_x(y), diff_y(y), diff_z(y), own[y] * STEP_DUAL])
        shrink(y, dual[0, y] + mm[0], dual[1, y] + mm[1], dual[2, y] + mm[2])
        sign(y, mm[3])

    def send_faces(rows):
        for y, face in zip(rows, drop(0, [dual[0, y] for y in rows])):
            hx2_s[y] = face * keep_x
        for y in rows:
            sent_f["hx", y] = Message(hx2_s.at[y, real, :], hx2_r.at[y, real, :], ff, y, to_xp, has_xp, has_xm)

    sent_f["hy"] = Message(hy2_s.at[real, :], hy2_r.at[real, :], ff, 8, to_yp, has_yp, has_ym, False)
    sent_f["hx", 7] = Message(hx2_s.at[7, real, :], hx2_r.at[7, real, :], ff, 7, to_xp, has_xp, has_xm, False)

    def last_again():
        for key in ("hx7", ("ep", 3), "epy", "hxd"):
            sent_b[key].arrived()
        finish(7)
        ey[...] = epy_r[...] - 2.0 * STEP_PRIMAL * rdy[...] * (hy_s[...] + hxd_r[...])
        forward(7)
        across, face = drop(1, [dual[1, 7], dual[0, 7]])
        hy2_s[...] = across * keep_y
        hx2_s[7] = face * keep_x
        sent_f["hy"].go()
        sent_f["hx", 7].go()

    pl.when(far_below)(last_again)
    pair_here(0)
    pair_here(1)
    for y in (1, 2, 3):
        finish(y)
    forward(1)
    forward(2)
    send_faces((1, 2))
    pair_here(2)
    finish(4)
    finish(5)
    forward(3)
    forward(4)
    send_faces((3, 4))
    pl.when(jnp.logical_not(far_below))(last_again)
    sent_b["hx", 3].arrived()
    finish(6)
    forward(5)
    forward(6)
    send_faces((5, 6))
    sent_b["hy"].arrived()
    sent_b["hyd"].arrived()
    finish(0)
    forward(0)
    send_faces((0,))

    for p in range(4):
        ya, yb = 2 * p, 2 * p + 1
        harms = drop(p % 2, [inner(ya), inner(yb)])
        for y, harm in ((ya, harms[0]), (yb, harms[1])):
            up[y] = advance(y, harm - hx2_s[y])
    for key in sent_b:
        sent_b[key].left()

    for y in (1, 2, 3, 4, 5, 6, 7, 0):
        sent_f["hx", y].arrived()
        face = hx2_r[y]
        if y == 0:
            sent_f["hy"].arrived()
            face = face + hy2_r[...]
        c_new = up[y] - STEP_PRIMAL * rdiv[y] * face
        cout[y] = c_new
        eout[y] = 2.0 * c_new - cur[y]
    for key in sent_f:
        sent_f[key].left()


def write_kernel(dual, cnew, enew, c_o, e_o, dg_o, ds_o, sem):
    copies = []
    for y in range(Y):
        for a in range(4):
            dst = dg_o.at[a] if a < 3 else ds_o
            copies.append((dual.at[a, y, pl.ds(0, N), :], dst.at[:, y, :]))
        copies.append((cnew.at[y, pl.ds(0, C), :], c_o.at[:, y, :]))
        copies.append((enew.at[y, pl.ds(0, C), :], e_o.at[:, y, :]))
    copies = [pltpu.make_async_copy(src, dst, sem.at[i]) for i, (src, dst) in enumerate(copies)]
    for copy in copies:
        copy.start()
    for copy in copies:
        copy.wait()


def per_device(signal, response, basis, mask, coefficients, extrapolated, dual_grad, dual_sign):
    block = pltpu.VMEM((Y, CP, Z), F32)
    face = pltpu.VMEM((CP, Z), F32)
    dma = pltpu.SemaphoreType.DMA
    dual, cnew, enew = pl.pallas_call(
        main_kernel,
        out_shape=(pltpu.VMEM((4, Y, NP, Z), F32), pltpu.VMEM((Y, CP, Z), F32), pltpu.VMEM((Y, CP, Z), F32)),
        in_specs=[HBM] * 8,
        out_specs=(VM, VM, VM),
        scratch_shapes=[
            block, block, face, block, block, block, block, block, face, block,
            pltpu.VMEM((Y, Z), jnp.int32), pltpu.VMEM((Y, Z), jnp.int32), pltpu.VMEM((Y, Z), jnp.int32),
            pltpu.VMEM((C, N), F32), pltpu.VMEM((1, C), F32),
            pltpu.VMEM((NP, 256), BF16), pltpu.VMEM((2 * CP, 768), BF16),
            pltpu.VMEM((2, 256, 4 * Z), BF16), pltpu.VMEM((2, 768, 2 * Z), BF16),
            block, block, face, block, block, face, face, face, face, block, face, block, face,
            dma((27,)), dma((Y, 4)), dma((7,)), dma((7,)), dma((13,)), dma((13,)), dma((9,)), dma((9,)),
            pltpu.SemaphoreType.REGULAR, pltpu.SemaphoreType.REGULAR,
        ],
        compiler_params=pltpu.CompilerParams(collective_id=0, has_side_effects=True, vmem_limit_bytes=40 * 2**20),
        name="steps",
    )(*(pltpu.with_memory_space_constraint(value, pltpu.HBM) for value in (
        signal.reshape(C, Y, Z), response.reshape(1, C), basis.T, mask.reshape(Y, Z), coefficients.reshape(C, Y, Z),
        extrapolated.reshape(C, Y, Z), dual_grad.reshape(3, N, Y, Z), dual_sign.reshape(N, Y, Z),
    )))
    c_o, e_o, dg_o, ds_o = pl.pallas_call(
        write_kernel,
        out_shape=(jax.ShapeDtypeStruct((C, Y, Z), F32), jax.ShapeDtypeStruct((C, Y, Z), F32),
                   jax.ShapeDtypeStruct((3, N, Y, Z), F32), jax.ShapeDtypeStruct((N, Y, Z), F32)),
        in_specs=[VM] * 3,
        out_specs=(HBM,) * 4,
        scratch_shapes=[dma((6 * Y,))],
        compiler_params=pltpu.CompilerParams(vmem_limit_bytes=16 * 2**20),
        name="write",
    )(*(pltpu.with_memory_space_constraint(value, pltpu.VMEM) for value in (dual, cnew, enew)))
    return (c_o.reshape(coefficients.shape), e_o.reshape(coefficients.shape),
            dg_o.reshape(dual_grad.shape), ds_o.reshape(dual_sign.shape))


def solution(mesh):
    in_specs = (
        P(None, "gx", "gy", None), P(), P(), P("gx", "gy", None), P(None, "gx", "gy", None),
        P(None, "gx", "gy", None), P(None, None, "gx", "gy", None), P(None, "gx", "gy", None),
    )
    out_specs = (
        P(None, "gx", "gy", None), P(None, "gx", "gy", None), P(None, None, "gx", "gy", None), P(None, "gx", "gy", None),
    )
    return jax.shard_map(per_device, mesh=mesh, in_specs=in_specs, out_specs=out_specs, check_vma=False)
```

```python
import jax
import jax.numpy as jnp
from jax import lax
from jax.experimental import pallas as pl
from jax.experimental.pallas import tpu as pltpu
from jax.sharding import PartitionSpec as P

STEP_PRIMAL = 0.25
STEP_DUAL = 0.02
TV_WEIGHT = 0.5

C, CP = 45, 48
N, NP = 362, 368
Y, Z = 8, 128
F32, BF16 = jnp.float32, jnp.bfloat16
MESH = pl.DeviceIdType.MESH
HBM = pl.BlockSpec(memory_space=pltpu.HBM)
VM = pl.BlockSpec(memory_space=pltpu.VMEM)


def halves(value):
    high = value.astype(BF16)
    return high, (value - high.astype(F32)).astype(BF16)


def main_kernel(sig, resp, bas, mask, coef, ext, dg, ds,
                dual, cout, eout,
                own, ex, ey, cur, sg, tgt, rdiv, rdx, rdy, up,
                mown, mx, my, bas_v, resp_v, fwd_w, bwd_w, q, r,
                ep_s, hx_s, hy_s, ep_r, hx_r, epy_r, hxd_r, hyd_r, hy_r, hx2_s, hy2_s, hx2_r, hy2_r,
                load_sem, dual_sem, a_s, a_r, b_s, b_r, f_s, f_r, ready, ready_d):
    gx, gy = lax.axis_index("gx"), lax.axis_index("gy")
    nx, ny = lax.axis_size("gx"), lax.axis_size("gy")
    has_xp, has_xm, has_yp, has_ym = gx < nx - 1, gx > 0, gy < ny - 1, gy > 0
    to_xp, to_xm, to_yp, to_ym = (gx + 1, gy), (gx - 1, gy), (gx, gy + 1), (gx, gy - 1)
    up_left, down_right = (gx - 1, gy + 1), (gx + 1, gy - 1)
    has_ul, has_dr = jnp.logical_and(has_xm, has_yp), jnp.logical_and(has_xp, has_ym)
    far_above = jnp.logical_and(lax.rem(gx, 8) == 7, has_xp)
    far_below = jnp.logical_and(lax.rem(gx, 8) == 0, has_xm)
    keep_x = jnp.where(has_xp, 1.0, 0.0).astype(F32)
    keep_y = jnp.where(has_yp, 1.0, 0.0).astype(F32)

    odd = lax.rem(gy, 2) == 1
    even = jnp.logical_not(odd)
    head = lax.rem(gx, 8) == 0
    tail = jnp.logical_or(lax.rem(gx, 8) == 7, gx == nx - 1)
    barrier = pltpu.get_barrier_semaphore()

    def both(*flags):
        out = flags[0]
        for flag in flags[1:]:
            out = jnp.logical_and(out, flag)
        return out

    def greet(sem, when, where):
        @pl.when(when)
        def _():
            pl.semaphore_signal(sem, inc=1, device_id=where, device_id_type=MESH)

    greet(barrier, has_xp, to_xp)
    greet(barrier, both(even, has_yp), to_yp)
    greet(barrier, both(even, has_ym), to_ym)
    greet(barrier, both(even, has_dr), down_right)

    def rows_in(src, dst, base):
        return [pltpu.make_async_copy(src.at[:, y, :], dst.at[y, pl.ds(0, C), :], load_sem.at[base + y]) for y in range(Y)]
    ext_in = rows_in(ext, own, 0)
    cur_in = rows_in(coef, cur, 8)
    sig_in = rows_in(sig, sg, 16)
    bas_in = pltpu.make_async_copy(bas, bas_v, load_sem.at[24])
    resp_in = pltpu.make_async_copy(resp, resp_v, load_sem.at[25])
    mask_in = pltpu.make_async_copy(mask, mown, load_sem.at[26])
    dual_in = [[pltpu.make_async_copy((dg.at[a] if a < 3 else ds).at[:, y, :], dual.at[a, y, pl.ds(0, N), :], dual_sem.at[y, a])
                for a in range(4)] for y in range(Y)]
    for copy in ext_in + [mask_in, bas_in, resp_in]:
        copy.start()
    for copy in cur_in + sig_in:
        copy.start()
    for y in range(Y):
        for copy in dual_in[y]:
            copy.start()

    left, up_there = jnp.minimum(gx, 1), jnp.minimum(ny - 1 - gy, 1)

    @pl.when(jnp.logical_or(has_xm, odd))
    def _():
        pl.semaphore_wait(barrier, left + lax.rem(gy, 2) * (1 + up_there + left * up_there))

    greet(ready, both(odd, has_ul, jnp.logical_not(head)), up_left)
    greet(ready, both(odd, has_yp, tail), to_yp)
    greet(ready_d, both(odd, has_ul, head), up_left)

    for copy in ext_in:
        copy.wait()

    class Message:
        def __init__(self, src, dst, sems, at, where, goes, comes, now=True):
            self.goes, self.comes = goes, comes
            self.copy = pltpu.make_async_remote_copy(src_ref=src, dst_ref=dst, send_sem=sems[0].at[at], recv_sem=sems[1].at[at],
                                                     device_id=where, device_id_type=MESH)
            if now:
                self.go()

        def go(self):
            pl.when(self.goes)(self.copy.start)

        def arrived(self):
            pl.when(self.comes)(self.copy.wait_recv)

        def left(self):
            pl.when(self.goes)(self.copy.wait_send)

    real = pl.ds(0, C)
    ab = (a_s, a_r)
    sent_a = {}
    face_copy = pltpu.make_async_remote_copy(src_ref=own.at[0, real, :], dst_ref=ey.at[real, :], send_sem=a_s.at[4], recv_sem=a_r.at[4],
                                             device_id=to_ym, device_id_type=MESH)

    @pl.when(both(odd, has_ym))
    def _():
        face_copy.start()
    for p in (3, 0, 1, 2):
        two = pl.ds(2 * p, 2)
        sent_a[p] = Message(own.at[two, real, :], ex.at[two, real, :], ab, p, to_xm, has_xm, has_xp)

    zeros, face0 = jnp.zeros((Y, CP, Z), F32), jnp.zeros((CP, Z), F32)

    @pl.when(jnp.logical_not(has_xp))
    def _():
        ex[...] = zeros
        ep_r[...] = zeros
        mx[...] = jnp.zeros((Y, Z), jnp.int32)

    @pl.when(jnp.logical_not(has_xm))
    def _():
        hx_r[...] = zeros
        hx2_r[...] = zeros

    @pl.when(jnp.logical_not(has_yp))
    def _():
        ey[...] = face0
        epy_r[...] = face0
        my[...] = jnp.zeros((Y, Z), jnp.int32)

    @pl.when(jnp.logical_not(has_ym))
    def _():
        hy_r[...] = face0
        hy2_r[...] = face0

    @pl.when(jnp.logical_not(has_ul))
    def _():
        hxd_r[...] = face0

    @pl.when(jnp.logical_not(has_dr))
    def _():
        hyd_r[...] = face0

    bas_in.wait()
    b_hi, b_lo = halves(bas_v[...])
    k_at = lax.broadcasted_iota(jnp.int32, (C, 256), 0)
    l_at = lax.broadcasted_iota(jnp.int32, (C, 256), 1)
    sel_hi = jnp.where((l_at == k_at) | (l_at == k_at + CP), 1.0, 0.0).astype(BF16)
    sel_lo = jnp.where(l_at == k_at + 2 * CP, 1.0, 0.0).astype(BF16)
    turn = (((0,), (0,)), ((), ()))
    fwd_w[...] = jnp.zeros((NP, 256), BF16)
    fwd_w[0:N, :] = (lax.dot_general(b_hi, sel_hi, turn, preferred_element_type=F32)
                     + lax.dot_general(b_lo, sel_lo, turn, preferred_element_type=F32)).astype(BF16)
    bwd_w[...] = jnp.zeros((2 * CP, 768), BF16)
    bwd_w[0:C, 0:N] = b_hi
    bwd_w[0:C, NP:NP + N] = b_hi
    bwd_w[CP:CP + C, 0:N] = b_lo
    q[:, 3 * CP:256, :] = jnp.zeros((2, 256 - 3 * CP, 4 * Z), BF16)
    r[:, 2 * NP:768, :] = jnp.zeros((2, 768 - 2 * NP, 2 * Z), BF16)
    for a in range(4):
        for y in range(Y):
            dual[a, y, pl.ds(N, NP - N), :] = jnp.zeros((NP - N, Z), F32)
    resp_in.wait()
    eye_f = lax.broadcasted_iota(jnp.int32, (CP, C), 0) == lax.broadcasted_iota(jnp.int32, (CP, C), 1)
    resp_c = jnp.sum(jnp.where(eye_f, jnp.broadcast_to(resp_v[...], (CP, C)), 0.0), axis=1, keepdims=True)

    mask_in.wait()

    def recip(mask_row):
        m = jnp.broadcast_to(mask_row.astype(F32), (CP, Z))
        w = m * resp_c
        return 1.0 / (1.0 + STEP_PRIMAL * w * resp_c), w
    for copy in sig_in + cur_in:
        copy.wait()
    for y in range(Y):
        inv, w = recip(mown[y:y + 1, :])
        rdiv[y] = inv
        tgt[y] = STEP_PRIMAL * w * sg[y]

    pad_ok = lax.broadcasted_iota(jnp.int32, (CP, Z), 0) < C
    lane_last = lax.broadcasted_iota(jnp.int32, (1, Z), 1) == Z - 1
    z_keep = jnp.where(lane_last, 0.0, 1.0).astype(F32)

    def lift(slot, fields):
        for a, field in enumerate(fields):
            hi, lo = halves(jnp.where(pad_ok, field, 0.0))
            at = slice(a * Z, (a + 1) * Z)
            q[slot, 0:CP, at] = hi
            q[slot, CP:2 * CP, at] = lo
            q[slot, 2 * CP:3 * CP, at] = hi
        mm = jnp.dot(fwd_w[...], q[slot, :, 0:len(fields) * Z], preferred_element_type=F32)
        return [mm[:, a * Z:(a + 1) * Z] for a in range(len(fields))]

    def diff_x(y):
        return (ex[y] - own[y]) * (STEP_DUAL * keep_x)

    def diff_y(y):
        if y < Y - 1:
            return (own[y + 1] - own[y]) * STEP_DUAL
        return (ey[...] - own[y]) * (STEP_DUAL * keep_y)

    def diff_z(y):
        return (pltpu.roll(own[y], Z - 1, 1) - own[y]) * (STEP_DUAL * z_keep)

    def shrink(y, sx, sy, sz):
        scale = jnp.minimum(1.0, TV_WEIGHT * lax.rsqrt(sx * sx + sy * sy + sz * sz))
        dual[0, y] = sx * scale
        dual[1, y] = sy * scale
        dual[2, y] = sz * scale

    def sign(y, amp):
        dual[3, y] = jnp.minimum(0.0, dual[3, y] + amp)

    def drop(slot, values):
        for a, value in enumerate(values):
            hi, lo = halves(value)
            r[slot, 0:NP, a * Z:(a + 1) * Z] = hi
            r[slot, NP:2 * NP, a * Z:(a + 1) * Z] = lo
        res = jnp.dot(bwd_w[...], r[slot, :, 0:len(values) * Z], preferred_element_type=F32)
        res = res[0:CP] + res[CP:2 * CP]
        return [res[:, a * Z:(a + 1) * Z] for a in range(len(values))]

    def inner(y):
        across = dual[1, y]
        if y == Y - 1:
            across = across * keep_y
        deep = dual[2, y] * z_keep
        w = dual[3, y] - across - deep + pltpu.roll(deep, 1, 1)
        if y > 0:
            w = w + dual[1, y - 1]
        return w

    def advance(y, harm):
        return (cur[y] - STEP_PRIMAL * harm + tgt[y]) * rdiv[y]

    for y in range(Y):
        for copy in dual_in[y]:
            copy.wait()
    def alone(y):
        fields = [diff_z(y), own[y] * STEP_DUAL]
        if y < Y - 1:
            fields.append(diff_y(y))
        mm = lift(y % 2, fields)
        dual[2, y] = dual[2, y] + mm[0]
        sign(y, mm[1])
        if y < Y - 1:
            dual[1, y] = dual[1, y] + mm[2]
    for y in range(Y // 2):
        alone(y)

    @pl.when(both(even, has_ym))
    def _():
        pl.semaphore_wait(ready, 1)
        face_copy.start()
    sent_a["my"] = Message(mown, my, ab, 5, to_ym, has_ym, has_yp)
    sent_a["mx"] = Message(mown, mx, ab, 6, to_xm, has_xm, has_xp)
    for y in range(Y // 2, Y):
        alone(y)

    bb = (b_s, b_r)
    sent_b = {
        "hy": Message(hy_s.at[real, :], hy_r.at[real, :], bb, 8, to_yp, has_yp, has_ym, False),
        "hyd": Message(hy_s.at[real, :], hyd_r.at[real, :], bb, 9, up_left, has_ul, has_dr, False),
        "hx7": Message(hx_s.at[7, real, :], hx_r.at[7, real, :], bb, 12, to_xp, has_xp, has_xm, False),
    }

    def last_row():
        sent_a[3].arrived()
        pl.when(has_yp)(face_copy.wait_recv)
        mm = lift(1, [diff_x(7), diff_y(7)])
        shrink(7, dual[0, 7] + mm[0], dual[1, 7] + mm[1], dual[2, 7])
        across, face = drop(1, [dual[1, 7], dual[0, 7]])
        hy_s[...] = across * keep_y
        hx_s[7] = face * keep_x
        for key in ("hy", "hyd", "hx7"):
            sent_b[key].go()

    pl.when(far_above)(last_row)
    for p in range(4):
        ya, yb = 2 * p, 2 * p + 1
        two = pl.ds(ya, 2)
        if p == 3:
            pl.when(jnp.logical_not(far_above))(last_row)
            mm = lift(0, [diff_x(6)])
            shrink(6, dual[0, 6] + mm[0], dual[1, 6], dual[2, 6])
            hx_s[6] = drop(0, [dual[0, 6]])[0] * keep_x
        else:
            sent_a[p].arrived()
            mm = lift(0, [diff_x(ya), diff_x(yb)])
            for y, part in ((ya, mm[0]), (yb, mm[1])):
                shrink(y, dual[0, y] + part, dual[1, y], dual[2, y])
            for y, face in zip((ya, yb), drop(0, [dual[0, ya], dual[0, yb]])):
                hx_s[y] = face * keep_x
        for y, harm in zip((ya, yb), drop(1, [inner(ya), inner(yb)])):
            u = advance(y, harm - hx_s[y])
            up[y] = u
            ep_s[y] = 2.0 * u - cur[y]
        if p == 0:
            sent_b["epy"] = Message(ep_s.at[0, real, :], epy_r.at[real, :], bb, 10, to_ym, has_ym, has_yp)
            @pl.when(both(even, has_dr, tail))
            def _():
                pl.semaphore_wait(ready_d, 1)
            sent_b["hxd"] = Message(hx_s.at[0, real, :], hxd_r.at[real, :], bb, 11, down_right, has_dr, has_ul)
        if p < 3:
            sent_b["hx", p] = Message(hx_s.at[two, real, :], hx_r.at[two, real, :], bb, p, to_xp, has_xp, has_xm)
        else:
            sent_b["hx", p] = Message(hx_s.at[6, real, :], hx_r.at[6, real, :], bb, p, to_xp, has_xp, has_xm)
        sent_b["ep", p] = Message(ep_s.at[two, real, :], ep_r.at[two, real, :], bb, 4 + p, to_xm, has_xm, has_xp)

    sent_a["mx"].arrived()
    sent_a["my"].arrived()
    for y in range(Y):
        rdx[y] = recip(mx[y:y + 1, :])[0]
    rdy[...] = recip(my[0:1, :])[0]
    pl.when(has_ym)(face_copy.wait_send)
    for key in sent_a:
        sent_a[key].left()

    def pair_here(p):
        sent_b["hx", p].arrived()
        sent_b["ep", p].arrived()

    def finish(y):
        face = hx_r[y]
        above = hx_s[y]
        if y == 0:
            face = face + hy_r[...]
            above = above + hyd_r[...]
        c_new = up[y] - STEP_PRIMAL * rdiv[y] * face
        own[y] = 2.0 * c_new - cur[y]
        cur[y] = c_new
        ex[y] = ep_r[y] - 2.0 * STEP_PRIMAL * rdx[y] * above

    ff = (f_s, f_r)
    sent_f = {}

    def forward(y):
        mm = lift(y % 2, [diff_x(y), diff_y(y), diff_z(y), own[y] * STEP_DUAL])
        shrink(y, dual[0, y] + mm[0], dual[1, y] + mm[1], dual[2, y] + mm[2])
        sign(y, mm[3])

    def send_faces(rows):
        for y, face in zip(rows, drop(0, [dual[0, y] for y in rows])):
            hx2_s[y] = face * keep_x
        for y in rows:
            sent_f["hx", y] = Message(hx2_s.at[y, real, :], hx2_r.at[y, real, :], ff, y, to_xp, has_xp, has_xm)

    sent_f["hy"] = Message(hy2_s.at[real, :], hy2_r.at[real, :], ff, 8, to_yp, has_yp, has_ym, False)
    sent_f["hx", 7] = Message(hx2_s.at[7, real, :], hx2_r.at[7, real, :], ff, 7, to_xp, has_xp, has_xm, False)

    def last_again():
        for key in ("hx7", ("ep", 3), "epy", "hxd"):
            sent_b[key].arrived()
        finish(7)
        ey[...] = epy_r[...] - 2.0 * STEP_PRIMAL * rdy[...] * (hy_s[...] + hxd_r[...])
        forward(7)
        across, face = drop(1, [dual[1, 7], dual[0, 7]])
        hy2_s[...] = across * keep_y
        hx2_s[7] = face * keep_x
        sent_f["hy"].go()
        sent_f["hx", 7].go()

    pl.when(far_below)(last_again)
    pair_here(0)
    pair_here(1)
    for y in (1, 2, 3):
        finish(y)
    forward(1)
    forward(2)
    send_faces((1, 2))
    pair_here(2)
    finish(4)
    finish(5)
    forward(3)
    forward(4)
    send_faces((3, 4))
    pl.when(jnp.logical_not(far_below))(last_again)
    sent_b["hx", 3].arrived()
    finish(6)
    forward(5)
    forward(6)
    send_faces((5, 6))

    def settle(p):
        ya, yb = 2 * p, 2 * p + 1
        for y, harm in zip((ya, yb), drop(p % 2, [inner(ya), inner(yb)])):
            up[y] = advance(y, harm - hx2_s[y])

    def settle_middle():
        settle(1)
        settle(2)
    pl.when(jnp.logical_not(far_above))(settle_middle)
    sent_b["hy"].arrived()
    sent_b["hyd"].arrived()
    finish(0)
    forward(0)
    send_faces((0,))

    settle(0)
    settle(3)
    pl.when(far_above)(settle_middle)
    for key in sent_b:
        sent_b[key].left()

    for y in (1, 2, 3, 4, 5, 6, 7, 0):
        sent_f["hx", y].arrived()
        face = hx2_r[y]
        if y == 0:
            sent_f["hy"].arrived()
            face = face + hy2_r[...]
        c_new = up[y] - STEP_PRIMAL * rdiv[y] * face
        cout[y] = c_new
        eout[y] = 2.0 * c_new - cur[y]
    for key in sent_f:
        sent_f[key].left()


def write_kernel(dual, cnew, enew, c_o, e_o, dg_o, ds_o, sem):
    copies = []
    for y in range(Y):
        for a in range(4):
            dst = dg_o.at[a] if a < 3 else ds_o
            copies.append((dual.at[a, y, pl.ds(0, N), :], dst.at[:, y, :]))
        copies.append((cnew.at[y, pl.ds(0, C), :], c_o.at[:, y, :]))
        copies.append((enew.at[y, pl.ds(0, C), :], e_o.at[:, y, :]))
    copies = [pltpu.make_async_copy(src, dst, sem.at[i]) for i, (src, dst) in enumerate(copies)]
    for copy in copies:
        copy.start()
    for copy in copies:
        copy.wait()


def per_device(signal, response, basis, mask, coefficients, extrapolated, dual_grad, dual_sign):
    block = pltpu.VMEM((Y, CP, Z), F32)
    face = pltpu.VMEM((CP, Z), F32)
    dma = pltpu.SemaphoreType.DMA
    dual, cnew, enew = pl.pallas_call(
        main_kernel,
        out_shape=(pltpu.VMEM((4, Y, NP, Z), F32), pltpu.VMEM((Y, CP, Z), F32), pltpu.VMEM((Y, CP, Z), F32)),
        in_specs=[HBM] * 8,
        out_specs=(VM, VM, VM),
        scratch_shapes=[
            block, block, face, block, block, block, block, block, face, block,
            pltpu.VMEM((Y, Z), jnp.int32), pltpu.VMEM((Y, Z), jnp.int32), pltpu.VMEM((Y, Z), jnp.int32),
            pltpu.VMEM((C, N), F32), pltpu.VMEM((1, C), F32),
            pltpu.VMEM((NP, 256), BF16), pltpu.VMEM((2 * CP, 768), BF16),
            pltpu.VMEM((2, 256, 4 * Z), BF16), pltpu.VMEM((2, 768, 2 * Z), BF16),
            block, block, face, block, block, face, face, face, face, block, face, block, face,
            dma((27,)), dma((Y, 4)), dma((7,)), dma((7,)), dma((13,)), dma((13,)), dma((9,)), dma((9,)),
            pltpu.SemaphoreType.REGULAR, pltpu.SemaphoreType.REGULAR,
        ],
        compiler_params=pltpu.CompilerParams(collective_id=0, has_side_effects=True, vmem_limit_bytes=40 * 2**20),
        name="steps",
    )(*(pltpu.with_memory_space_constraint(value, pltpu.HBM) for value in (
        signal.reshape(C, Y, Z), response.reshape(1, C), basis.T, mask.reshape(Y, Z), coefficients.reshape(C, Y, Z),
        extrapolated.reshape(C, Y, Z), dual_grad.reshape(3, N, Y, Z), dual_sign.reshape(N, Y, Z),
    )))
    c_o, e_o, dg_o, ds_o = pl.pallas_call(
        write_kernel,
        out_shape=(jax.ShapeDtypeStruct((C, Y, Z), F32), jax.ShapeDtypeStruct((C, Y, Z), F32),
                   jax.ShapeDtypeStruct((3, N, Y, Z), F32), jax.ShapeDtypeStruct((N, Y, Z), F32)),
        in_specs=[VM] * 3,
        out_specs=(HBM,) * 4,
        scratch_shapes=[dma((6 * Y,))],
        compiler_params=pltpu.CompilerParams(vmem_limit_bytes=16 * 2**20),
        name="write",
    )(*(pltpu.with_memory_space_constraint(value, pltpu.VMEM) for value in (dual, cnew, enew)))
    return (c_o.reshape(coefficients.shape), e_o.reshape(coefficients.shape),
            dg_o.reshape(dual_grad.shape), ds_o.reshape(dual_sign.shape))


def solution(mesh):
    in_specs = (
        P(None, "gx", "gy", None), P(), P(), P("gx", "gy", None), P(None, "gx", "gy", None),
        P(None, "gx", "gy", None), P(None, None, "gx", "gy", None), P(None, "gx", "gy", None),
    )
    out_specs = (
        P(None, "gx", "gy", None), P(None, "gx", "gy", None), P(None, None, "gx", "gy", None), P(None, "gx", "gy", None),
    )
    return jax.shard_map(per_device, mesh=mesh, in_specs=in_specs, out_specs=out_specs, check_vma=False)
```
